32 devices in a mesh: blk: 32 (over z, y, x, core).
Axes of the slice: x: 2, y: 2, z: 4, core: 2. Of those that a mesh axis runs over, the one named last changes fastest.
Arguments:
- tensor_blocks: bfloat16 [352, 32, 32, 1024], P('blk')
- block_index: int32 [352, 4], P('blk'), may hold values from 0 to 8, as said below
- starts: float32 [256, 32], P(None, 'blk'), may hold values from -6 to 6
- shifts: float32 [32], replicated, may hold values from 0.5 to 2
Outputs:
- iterate: float32 [256, 32], P(None, 'blk')
- estimate: float32 [32], P('blk')
The draws below stay inside these ranges and needn't reach their ends.
Inputs may be any that keep to these rules, and one draw needn't show every extreme that they name: `block_index`: every sorted quadruple i <= j <= k <= l of 0 to 7 is held by exactly one slot; every other slot holds 8 in all four entries and is not used. A live slot's block is unchanged when two of its axes with equal block indices are swapped.
All inputs are finite; a program needn't handle non-finite values.
Results may differ from the reference program's by a relative error of at most 0.009.
Values sent between devices are 32-bit elements; how exact they have to be, the bound alone decides.
No kernel may reach another device: no remote copies, remote signals or barrier semaphores. Data moves between devices by JAX's collectives and lax.ppermute only.
A program may use at most 192 MiB of HBM per device.

```python
import math
import jax
import jax.numpy as jnp
import numpy as np
from jax import lax

NSIZE = 256
BS = 32
ITERS = 2
SLOTS = 352
STARTS = 32


def quadruple_table(count):
    rows_list = []
    for first in range(count):
        for second in range(first, count):
            for third in range(second, count):
                for fourth in range(third, count):
                    rows_list.append([first, second, third, fourth])
    return np.array(rows_list, dtype=np.int32)


def orderings():
    listing = []
    for first in range(4):
        for second in range(4):
            for third in range(4):
                for fourth in range(4):
                    if len(set([first, second, third, fourth])) == 4:
                        listing.append((first, second, third, fourth))
    return listing


def slot_table(key):
    count = NSIZE // BS
    quadruples = jnp.asarray(quadruple_table(count))
    order = jax.random.permutation(jax.random.fold_in(key, 7), SLOTS)
    table = jnp.full((SLOTS, 4), count, jnp.int32)
    return table.at[order[:quadruples.shape[0]]].set(quadruples)


def draw_block_index(key, part):
    return slot_table(key)


def draw_tensor_blocks(key, part):
    table = slot_table(key)
    slot_keys = jax.random.split(jax.random.fold_in(key, 11), SLOTS)
    listing = orderings()
    scale_value = float(NSIZE) ** (-1.5)

    def make_slot(item):
        slot_key, indices = item
        raw_values = jax.random.normal(slot_key, (BS, BS, BS, BS), jnp.float32)
        total = jnp.zeros((BS, BS, BS, BS), jnp.float32)
        matched = jnp.float32(0.0)
        for ordering in listing:
            moved = jnp.stack([indices[ordering[0]], indices[ordering[1]], indices[ordering[2]], indices[ordering[3]]])
            agree = jnp.all(moved == indices).astype(jnp.float32)
            total = total + agree * jnp.transpose(raw_values, ordering)
            matched = matched + agree
        block = total / matched * scale_value
        return block.reshape(BS, BS, BS * BS).astype(jnp.bfloat16)
    return lax.map(make_slot, (slot_keys, table))


def level_of(own_key, shape, shards, least, high):
    def one(dim, blocks):
        heights = jax.random.uniform(jax.random.fold_in(jax.random.fold_in(own_key, 6), dim), (blocks,), jnp.float32, least / len(shards), high / len(shards))
        return jnp.repeat(jnp.exp(heights), shape[dim] // blocks).reshape((-1,) + (1,) * (len(shape) - dim - 1))

    gain = one(*shards[0])
    for cut in shards[1:]:
        gain = gain * one(*cut)
    return gain


def bell_draw(rng, extent, spread, bound, cuts=(), kind=jnp.bfloat16):
    entries = jax.random.normal(rng, extent, jnp.float32) * spread
    if len(cuts) > 0:
        entries = level_of(rng, extent, cuts, -0.22, 0.18) * entries
    return jnp.clip(entries, min=-bound, max=bound).astype(kind)


def setup_inputs(seed: int = 0) -> dict:
    streams_of = jax.random.split(jax.random.key(seed), 5)
    return {
        "tensor_blocks": draw_tensor_blocks(jax.random.fold_in(streams_of[4], 71), 0),
        "block_index": draw_block_index(jax.random.fold_in(streams_of[4], 71), 0),
        "starts": bell_draw(streams_of[2], (NSIZE, STARTS), 1.0, 6.0, ((1, 32),), jnp.float32),
        "shifts": jnp.clip(jnp.exp(jax.random.uniform(streams_of[3], (STARTS,), jnp.float32, math.log(0.5), math.log(2.0))), 0.5, 2.0),
    }


letters = 'abcd'

def normalize(values):
    return values * lax.rsqrt(lax.optimization_barrier(jnp.mean(values * values, axis=0)) + 1e-06)

def factor_product(indices):
    product = jnp.float32(1.0)
    for other in range(1, 4):
        earlier = jnp.float32(0.0)
        for before in range(other):
            earlier = earlier + (indices[before] == indices[other]).astype(jnp.float32)
        product = product * (1.0 + earlier)
    return product

def contract_axis(tensor, pieces, position):
    others = [other for other in range(4) if other != position]
    leading = others[0]
    paired = (pieces[others[1]][:, None, :] * pieces[others[2]][None, :, :]).astype(jnp.bfloat16)
    kept = ''.join(sorted(letters[position] + letters[leading]))
    pattern = 'abcd,' + letters[others[1]] + letters[others[2]] + 'r->' + kept + 'r'
    partial_sum = jnp.einsum(pattern, tensor.astype(jnp.float32), paired.astype(jnp.float32), precision=lax.Precision.HIGHEST)
    if position < leading:
        return lax.optimization_barrier(jnp.sum(partial_sum * pieces[leading][None, :, :], axis=1))
    return lax.optimization_barrier(jnp.sum(partial_sum * pieces[leading][:, None, :], axis=0))

def apply_tensor(tensor_blocks, block_index, current):
    blocks_count = NSIZE // BS

    def one_slot(total, item):
        merged, indices = item
        tensor = merged.reshape(BS, BS, BS, BS)
        live = (indices[0] < blocks_count).astype(jnp.float32)
        safe = jnp.minimum(indices, blocks_count - 1).astype(jnp.int32)
        pieces = [lax.dynamic_slice_in_dim(current, safe[other] * BS, BS, 0) for other in range(4)]
        weight = live * 6.0 / factor_product(indices)
        for position in range(4):
            result = weight * contract_axis(tensor, pieces, position)
            start = safe[position] * BS
            total = lax.dynamic_update_slice_in_dim(total, lax.dynamic_slice_in_dim(total, start, BS, 0) + result, start, 0)
        return (total, None)
    total, unused = lax.scan(one_slot, jnp.zeros(current.shape, jnp.float32), (tensor_blocks, block_index))
    return total

def reference(tensor_blocks, block_index, starts, shifts):
    current = normalize(starts)
    previous = current
    applied = current
    for step_id in range(ITERS):
        applied = apply_tensor(tensor_blocks, block_index, current)
        previous = current
        current = normalize(applied + shifts[None, :] * current)
    estimate = lax.optimization_barrier(jnp.mean(previous * applied, axis=0)) * lax.rsqrt(lax.optimization_barrier(jnp.mean(applied * applied, axis=0)) + 1e-06)
    return (current, estimate)
```

```python
import functools

import jax
import jax.numpy as jnp
from jax import lax
from jax.experimental import pallas as pl
from jax.experimental.pallas import tpu as pltpu
from jax.sharding import PartitionSpec as P

ITERS = 2
EPS = 1e-06


def normalize_rows(values):
    return values * lax.rsqrt(jnp.mean(values * values, axis=1, keepdims=True) + EPS)


def split_terms(values, count):
    terms = []
    rest = values
    for unused in range(count):
        term = rest.astype(jnp.bfloat16)
        terms.append(term)
        rest = rest - term.astype(jnp.float32)
    return terms


def dot_rows(left, right):
    return jnp.dot(left, right, preferred_element_type=jnp.float32)


def mixed_rows(ins, shape):
    values = ins[0][...].reshape(shape)
    if len(ins) > 1:
        values = ins[1][...] * values
        image = ins[2][...]
        for term in ins[3:]:
            image = image + term[...]
        values = image + values
    return normalize_rows(values)


def slot_weight(raw):
    factor = jnp.float32(1.0)
    for axis in range(1, 4):
        earlier = jnp.float32(1.0)
        for before in range(axis):
            earlier = earlier + jnp.where(raw[before] == raw[axis], 1.0, 0.0).astype(jnp.float32)
        factor = factor * earlier
    return jnp.full((1, 1), 6.0, jnp.float32) / jnp.full((1, 1), factor, jnp.float32)


def apply_kernel(index_ref, blocks_ref, *refs, blocks, size, parts, inputs):
    ins, refs = refs[:inputs], refs[inputs:]
    y_ref, x_ref, matrix_ref, rep_ref, tile_ref, wide_ref, fold_ref, sems = refs
    slots, pairs = matrix_ref.shape[:2]
    starts = x_ref.shape[0]
    lanes = tile_ref.shape[2]
    repeats = pairs // lanes
    height = pairs // parts

    def copy(slot, part):
        rows = pl.ds(part * height, height)
        return pltpu.make_async_copy(
            blocks_ref.at[slot, rows], matrix_ref.at[slot, rows], sems.at[slot, part]
        )

    ahead = min(3, slots)
    for slot in range(ahead):
        for part in range(parts):
            copy(slot, part).start()

    current = mixed_rows(ins, x_ref.shape)
    x_ref[...] = current
    wide_ref[...] = jnp.zeros_like(wide_ref)
    fold_ref[...] = jnp.zeros_like(fold_ref)
    stacked = jnp.concatenate([current[:, block * size:(block + 1) * size] for block in range(blocks)], axis=0)
    terms = jnp.concatenate(split_terms(stacked, 3), axis=1)
    rows = lax.broadcasted_iota(jnp.int32, (3 * size, pairs), 0) % size
    cols = lax.broadcasted_iota(jnp.int32, (3 * size, pairs), 1)
    spread = jnp.where(cols // size == rows, 1.0, 0.0).astype(jnp.bfloat16)
    cycle = jnp.where(cols % size == rows, 1.0, 0.0)[:, :lanes].astype(jnp.bfloat16)
    rep_ref[...] = dot_rows(terms, spread).reshape(rep_ref.shape)
    tile_ref[...] = dot_rows(terms, cycle).reshape(tile_ref.shape)

    def one_slot(slot, carry):
        raw = [index_ref[slot * 4 + axis] for axis in range(4)]
        @pl.when(slot + ahead < slots)
        def _():
            for part in range(parts):
                copy(slot + ahead, part).start()

        for part in range(parts):
            copy(slot, part).wait()

        @pl.when(raw[0] < blocks)
        def _():
            first, second, third, fourth = raw
            weight = slot_weight(raw)
            matrix = matrix_ref[slot]

            def pair(left, right):
                cycled = jnp.tile(tile_ref[right], (1, repeats))
                return (rep_ref[left] * cycled).astype(jnp.bfloat16)

            def spread_out(image, left, right):
                image = image * weight
                wide_ref[left] += image * jnp.tile(tile_ref[right], (1, repeats))
                scaled = image * rep_ref[left]
                folded = scaled[:, :lanes]
                for part in range(1, repeats):
                    folded = folded + scaled[:, part * lanes:(part + 1) * lanes]
                fold_ref[right] += folded

            late = pair(third, fourth)
            early = pair(first, second)
            upper = lax.dot_general(
                late, matrix, (((1,), (1,)), ((), ())), preferred_element_type=jnp.float32
            )
            lower = dot_rows(early, matrix)
            spread_out(upper, first, second)
            spread_out(lower, third, fourth)

        return carry

    lax.fori_loop(0, slots, one_slot, 0)

    rows = lax.broadcasted_iota(jnp.int32, (pairs, size), 0)
    cols = lax.broadcasted_iota(jnp.int32, (pairs, size), 1)
    gather = jnp.where(rows // size == cols, 1.0, 0.0).astype(jnp.bfloat16)
    wrap = jnp.where(rows % size == cols, 1.0, 0.0)[:lanes].astype(jnp.bfloat16)
    total = jnp.zeros((blocks * starts, size), jnp.float32)
    for term in split_terms(wide_ref[...].reshape(blocks * starts, pairs), 2):
        total = total + dot_rows(term, gather)
    for term in split_terms(fold_ref[...].reshape(blocks * starts, lanes), 2):
        total = total + dot_rows(term, wrap)
    for block in range(blocks):
        span = slice(block * size, (block + 1) * size)
        y_ref[..., span] = total[block * starts:(block + 1) * starts].reshape(y_ref.shape[:-1] + (size,))


def packed_kernel(index_ref, blocks_ref, *refs, blocks, size, ahead, parts, inputs):
    ins, refs = refs[:inputs], refs[inputs:]
    y_ref, x_ref, matrix_ref, rows_ref, lead_ref, right_ref, left_ref, lead_sum_ref, row_sum_ref, sems = refs
    slots, pairs = matrix_ref.shape[:2]
    starts, order = x_ref.shape
    lanes = rows_ref.shape[2]
    groups = lanes // starts
    local = size // groups
    tile = pairs // groups
    height = pairs // parts

    def copy(slot, part):
        rows = pl.ds(part * height, height)
        return pltpu.make_async_copy(
            blocks_ref.at[slot, rows], matrix_ref.at[slot, rows], sems.at[slot, part]
        )

    def arrive(slot):
        if slot + ahead < slots:
            for part in range(parts):
                copy(slot + ahead, part).start()
        for part in range(parts):
            copy(slot, part).wait()

    for slot in range(min(ahead, slots)):
        for part in range(parts):
            copy(slot, part).start()

    group_of = lax.broadcasted_iota(jnp.int32, (1, lanes), 1) // starts

    current = mixed_rows(ins, x_ref.shape)
    x_ref[...] = current
    rows_ref[...] = jnp.concatenate([current] * groups, axis=0).T.reshape(rows_ref.shape)
    for block in range(blocks):
        lead = jnp.zeros((local, lanes), jnp.float32)
        for group in range(groups):
            lead = jnp.where(group_of == group, rows_ref[block, group * local:(group + 1) * local, :], lead)
        lead_ref[block] = lead
    lead_sum_ref[...] = jnp.zeros_like(lead_sum_ref)
    row_sum_ref[...] = jnp.zeros_like(row_sum_ref)

    def scatter(image, weight, left, right):
        inner = rows_ref[right] * weight
        outer = jnp.zeros((size, lanes), jnp.float32)
        for part in range(local):
            piece = image[part * size:(part + 1) * size]
            lead_sum_ref[left, part * 8:(part + 1) * 8, :] += jnp.sum(
                (piece * inner).reshape(size // 8, 8, lanes), axis=0
            )
            outer = outer + piece * lead_ref[left, part:part + 1, :]
        row_sum_ref[right] += outer * weight

    def body(wide_acc, thin_acc):
        for queue in range(2):
            for parity in range(2):
                pltpu.matmul_pop(wide_acc[queue][parity])
                for column in range(groups):
                    pltpu.matmul_pop(thin_acc[queue][parity][column])
        arrive(0)
        for slot in range(slots):
            parity = slot % 2
            raw = [index_ref[slot * 4 + axis] for axis in range(4)]
            live = jnp.where(raw[0] < blocks, 1.0, 0.0).astype(jnp.float32)
            first, second, third, fourth = [jnp.minimum(value, blocks - 1) for value in raw]
            weight = slot_weight(raw)
            inner = rows_ref[fourth] * live
            for row in range(size):
                right_ref[parity, row * size:(row + 1) * size, :] = (
                    rows_ref[third, row:row + 1, :] * inner
                ).astype(jnp.bfloat16)
            inner = rows_ref[second] * live
            packed = jnp.concatenate(
                [lead_ref[first, part:part + 1, :] * inner for part in range(local)], axis=0
            )
            left_ref[parity] = packed.T.astype(jnp.bfloat16)
            for half in range(groups // 2):
                for column in range(groups):
                    for queue in range(2):
                        line = 2 * half + queue
                        block = matrix_ref[slot, line * tile:(line + 1) * tile, column * tile:(column + 1) * tile]
                        right = right_ref[parity, column * tile:(column + 1) * tile, :]
                        right = jnp.where(group_of == line, right, jnp.zeros_like(right))
                        right = jnp.concatenate([right, jnp.zeros_like(right)], axis=1)
                        pltpu.matmul_push_rhs(right, staging_register=0, mxu_index=queue)
                        pltpu.matmul_acc_lhs(wide_acc[queue][parity], block, load_staged_rhs=0)
                        pltpu.matmul_push_rhs(block, staging_register=1, mxu_index=queue)
                        pltpu.matmul_acc_lhs(
                            thin_acc[queue][parity][column],
                            left_ref[parity, line * starts:(line + 1) * starts, :],
                            load_staged_rhs=1,
                        )
                if half == 0 and slot + 1 < slots:
                    arrive(slot + 1)
            upper = pltpu.matmul_pop(wide_acc[0][parity])[:, :lanes] + pltpu.matmul_pop(wide_acc[1][parity])[:, :lanes]
            lower = jnp.concatenate([
                pltpu.matmul_pop(thin_acc[0][parity][column]) + pltpu.matmul_pop(thin_acc[1][parity][column])
                for column in range(groups)
            ], axis=0)
            scatter(upper, weight, first, second)
            scatter(lower.T, weight, third, fourth)

    wide = [[pltpu.ACC(queue)((tile, tile), jnp.float32) for unused in range(2)] for queue in range(2)]
    thin = [
        [[pltpu.ACC(queue)((starts, tile), jnp.float32) for unused in range(groups)] for parity in range(2)]
        for queue in range(2)
    ]
    pl.run_scoped(body, wide, thin)

    for block in range(blocks):
        lead = jnp.sum(lead_sum_ref[block].reshape(local, 8, lanes), axis=1)
        for group in range(groups):
            row_sum_ref[block, group * local:(group + 1) * local, :] += jnp.where(group_of == group, lead, 0.0)
    spread = row_sum_ref[...].reshape(order, lanes).T
    total = spread[:starts]
    for group in range(1, groups):
        total = total + spread[group * starts:(group + 1) * starts]
    y_ref[...] = total.reshape(y_ref.shape)


def apply_tensor(blocks, index, arrays, starts, order, result):
    slots, pairs = blocks.shape[:2]
    size = int(round(pairs ** 0.5))
    count = order // size
    lanes = min(pairs, 128)
    parts = 1
    ahead = 4
    shape = jax.ShapeDtypeStruct((starts, order), jnp.float32)
    vmem = pl.BlockSpec(memory_space=pltpu.VMEM)
    groups = 128 // starts
    packed = starts % 16 == 0 and groups == 4 and pairs == 1024 and size == 32
    settings = dict(blocks=count, size=size, parts=parts, inputs=len(arrays))
    if packed:
        kernel = functools.partial(packed_kernel, ahead=ahead, **settings)
        scratch = [
            pltpu.VMEM((count, size, lanes), jnp.float32),
            pltpu.VMEM((count, size // groups, lanes), jnp.float32),
            pltpu.VMEM((2, pairs, lanes), jnp.bfloat16),
            pltpu.VMEM((2, lanes, pairs // groups), jnp.bfloat16),
            pltpu.VMEM((count, 8 * size // groups, lanes), jnp.float32),
            pltpu.VMEM((count, size, lanes), jnp.float32),
        ]
    else:
        kernel = functools.partial(apply_kernel, **settings)
        scratch = [
            pltpu.VMEM((count, starts, pairs), jnp.float32),
            pltpu.VMEM((count, starts, lanes), jnp.float32),
            pltpu.VMEM((count, starts, pairs), jnp.float32),
            pltpu.VMEM((count, starts, lanes), jnp.float32),
        ]
    return pl.pallas_call(
        kernel,
        out_shape=(jax.ShapeDtypeStruct(result, jnp.float32), shape),
        in_specs=[pl.BlockSpec(memory_space=pltpu.SMEM), pl.BlockSpec(memory_space=pl.ANY)] + [vmem] * len(arrays),
        out_specs=(vmem, vmem),
        scratch_shapes=[pltpu.VMEM((slots, pairs, pairs), jnp.bfloat16)]
        + scratch
        + [pltpu.SemaphoreType.DMA((slots, parts))],
        compiler_params=pltpu.CompilerParams(vmem_limit_bytes=56 * 1024 * 1024),
        name="apply_tensor",
    )(index, blocks, *arrays)


def finish_kernel(offset_ref, pieces_ref, current_ref, shifts_ref, iterate_ref, estimate_ref):
    own, order = iterate_ref.shape
    image = jnp.sum(pieces_ref[...], axis=0)
    rows = pl.ds(offset_ref[0], own)
    previous = current_ref[rows, :]
    iterate_ref[...] = normalize_rows(image + shifts_ref[rows, :] * previous)
    cosine = jnp.mean(previous * image, axis=1, keepdims=True)
    estimate_ref[...] = cosine * lax.rsqrt(jnp.mean(image * image, axis=1, keepdims=True) + EPS)


def finish(offset, pieces, current, shifts, own):
    order = pieces.shape[2]
    vmem = pl.BlockSpec(memory_space=pltpu.VMEM)
    return pl.pallas_call(
        finish_kernel,
        out_shape=(
            jax.ShapeDtypeStruct((own, order), jnp.float32),
            jax.ShapeDtypeStruct((own, 1), jnp.float32),
        ),
        in_specs=[pl.BlockSpec(memory_space=pltpu.SMEM), vmem, vmem, vmem],
        out_specs=(vmem, vmem),
        name="finish",
    )(offset, pieces, current, shifts)


def stage_sizes(devices):
    sizes = []
    rest = devices
    if rest % 2 == 0:
        sizes.append(2)
        rest //= 2
    while rest > 1:
        size = next(value for value in (4, 2, 3, 5, 7, rest) if rest % value == 0)
        sizes.append(size)
        rest //= size
    return sizes


def sum_terms(values, axis_name, devices):
    stride = 1
    terms = [values]
    for size in stage_sizes(devices):
        values = functools.reduce(jnp.add, terms)
        terms = [values]
        for step in range(1, size):
            moves = []
            for device in range(devices):
                digit = device // stride % size
                target = digit ^ step if size in (2, 4) else (digit + step) % size
                moves.append((device, device + (target - digit) * stride))
            terms.append(lax.ppermute(values, axis_name, moves))
        stride *= size
    return terms


def solution(mesh):
    devices = mesh.shape["blk"]

    def body(tensor_blocks, block_index, starts, shifts):
        slots, size = tensor_blocks.shape[:2]
        own_count = starts.shape[1]
        order = starts.shape[0]
        matrices = tensor_blocks.reshape(slots, size * size, size * size)
        index = block_index.reshape(slots * 4)
        offset = lax.axis_index("blk") * own_count
        total = devices * own_count
        column = shifts[:, None]
        pieces = (devices, own_count, order)
        copies = jnp.broadcast_to(starts.T[None], pieces)
        arrays = (lax.all_to_all(copies, "blk", 0, 0, tiled=True),)
        for step in range(ITERS):
            last = step == ITERS - 1
            applied, current = apply_tensor(
                matrices, index, arrays, total, order, pieces if last else (total, order)
            )
            if not last:
                arrays = (current, column, *sum_terms(applied, "blk", devices))
        received = lax.all_to_all(applied, "blk", 0, 0, tiled=True)
        iterate, estimate = finish(offset.reshape(1), received, current, column, own_count)
        return iterate.T, estimate[:, 0]

    placed = (P("blk", None, None, None), P("blk", None), P(None, "blk"), P())
    return jax.shard_map(
        body, mesh=mesh, in_specs=placed, out_specs=(P(None, "blk"), P("blk")), check_vma=False
    )
```

```python
import functools

import jax
import jax.numpy as jnp
from jax import lax
from jax.experimental import pallas as pl
from jax.experimental.pallas import tpu as pltpu
from jax.sharding import PartitionSpec as P

ITERS = 2
EPS = 1e-06


def normalize_rows(values):
    return values * lax.rsqrt(jnp.mean(values * values, axis=1, keepdims=True) + EPS)


def split_terms(values, count):
    terms = []
    rest = values
    for unused in range(count):
        term = rest.astype(jnp.bfloat16)
        terms.append(term)
        rest = rest - term.astype(jnp.float32)
    return terms


def dot_rows(left, right):
    return jnp.dot(left, right, preferred_element_type=jnp.float32)


def mixed_rows(ins, shape):
    values = ins[0][...].reshape(shape)
    if len(ins) > 1:
        values = ins[1][...] * values
        image = ins[2][...]
        for term in ins[3:]:
            image = image + term[...]
        values = image + values
    return normalize_rows(values)


def slot_weight(raw):
    factor = jnp.float32(1.0)
    for axis in range(1, 4):
        earlier = jnp.float32(1.0)
        for before in range(axis):
            earlier = earlier + jnp.where(raw[before] == raw[axis], 1.0, 0.0).astype(jnp.float32)
        factor = factor * earlier
    return jnp.full((1, 1), 6.0, jnp.float32) / jnp.full((1, 1), factor, jnp.float32)


def apply_kernel(index_ref, blocks_ref, *refs, blocks, size, parts, inputs):
    ins, refs = refs[:inputs], refs[inputs:]
    y_ref, x_ref, matrix_ref, rep_ref, tile_ref, wide_ref, fold_ref, sems = refs
    slots, pairs = matrix_ref.shape[:2]
    starts = x_ref.shape[0]
    lanes = tile_ref.shape[2]
    repeats = pairs // lanes
    height = pairs // parts

    def copy(slot, part):
        rows = pl.ds(part * height, height)
        return pltpu.make_async_copy(
            blocks_ref.at[slot, rows], matrix_ref.at[slot, rows], sems.at[slot, part]
        )

    ahead = min(3, slots)
    for slot in range(ahead):
        for part in range(parts):
            copy(slot, part).start()

    current = mixed_rows(ins, x_ref.shape)
    x_ref[...] = current
    wide_ref[...] = jnp.zeros_like(wide_ref)
    fold_ref[...] = jnp.zeros_like(fold_ref)
    stacked = jnp.concatenate([current[:, block * size:(block + 1) * size] for block in range(blocks)], axis=0)
    terms = jnp.concatenate(split_terms(stacked, 3), axis=1)
    rows = lax.broadcasted_iota(jnp.int32, (3 * size, pairs), 0) % size
    cols = lax.broadcasted_iota(jnp.int32, (3 * size, pairs), 1)
    spread = jnp.where(cols // size == rows, 1.0, 0.0).astype(jnp.bfloat16)
    cycle = jnp.where(cols % size == rows, 1.0, 0.0)[:, :lanes].astype(jnp.bfloat16)
    rep_ref[...] = dot_rows(terms, spread).reshape(rep_ref.shape)
    tile_ref[...] = dot_rows(terms, cycle).reshape(tile_ref.shape)

    def one_slot(slot, carry):
        raw = [index_ref[slot * 4 + axis] for axis in range(4)]
        @pl.when(slot + ahead < slots)
        def _():
            for part in range(parts):
                copy(slot + ahead, part).start()

        for part in range(parts):
            copy(slot, part).wait()

        @pl.when(raw[0] < blocks)
        def _():
            first, second, third, fourth = raw
            weight = slot_weight(raw)
            matrix = matrix_ref[slot]

            def pair(left, right):
                cycled = jnp.tile(tile_ref[right], (1, repeats))
                return (rep_ref[left] * cycled).astype(jnp.bfloat16)

            def spread_out(image, left, right):
                image = image * weight
                wide_ref[left] += image * jnp.tile(tile_ref[right], (1, repeats))
                scaled = image * rep_ref[left]
                folded = scaled[:, :lanes]
                for part in range(1, repeats):
                    folded = folded + scaled[:, part * lanes:(part + 1) * lanes]
                fold_ref[right] += folded

            late = pair(third, fourth)
            early = pair(first, second)
            upper = lax.dot_general(
                late, matrix, (((1,), (1,)), ((), ())), preferred_element_type=jnp.float32
            )
            lower = dot_rows(early, matrix)
            spread_out(upper, first, second)
            spread_out(lower, third, fourth)

        return carry

    lax.fori_loop(0, slots, one_slot, 0)

    rows = lax.broadcasted_iota(jnp.int32, (pairs, size), 0)
    cols = lax.broadcasted_iota(jnp.int32, (pairs, size), 1)
    gather = jnp.where(rows // size == cols, 1.0, 0.0).astype(jnp.bfloat16)
    wrap = jnp.where(rows % size == cols, 1.0, 0.0)[:lanes].astype(jnp.bfloat16)
    total = jnp.zeros((blocks * starts, size), jnp.float32)
    for term in split_terms(wide_ref[...].reshape(blocks * starts, pairs), 2):
        total = total + dot_rows(term, gather)
    for term in split_terms(fold_ref[...].reshape(blocks * starts, lanes), 2):
        total = total + dot_rows(term, wrap)
    for block in range(blocks):
        span = slice(block * size, (block + 1) * size)
        y_ref[..., span] = total[block * starts:(block + 1) * starts].reshape(y_ref.shape[:-1] + (size,))


def packed_kernel(index_ref, blocks_ref, *refs, blocks, size, ahead, parts, inputs):
    ins, refs = refs[:inputs], refs[inputs:]
    y_ref, x_ref, matrix_ref, rows_ref, lead_ref, right_ref, left_ref, lead_sum_ref, row_sum_ref, sems = refs
    slots, pairs = matrix_ref.shape[:2]
    starts, order = x_ref.shape
    lanes = rows_ref.shape[2]
    groups = lanes // starts
    local = size // groups
    tile = pairs // groups
    height = pairs // parts

    def copy(slot, part):
        rows = pl.ds(part * height, height)
        return pltpu.make_async_copy(
            blocks_ref.at[slot, rows], matrix_ref.at[slot, rows], sems.at[slot, part]
        )

    def arrive(slot, part):
        if slot + ahead < slots:
            copy(slot + ahead, part).start()
        copy(slot, part).wait()

    for slot in range(min(ahead, slots)):
        for part in range(parts):
            copy(slot, part).start()

    group_of = lax.broadcasted_iota(jnp.int32, (1, lanes), 1) // starts

    current = mixed_rows(ins, x_ref.shape)
    x_ref[...] = current
    rows_ref[...] = jnp.concatenate([current] * groups, axis=0).T.reshape(rows_ref.shape)
    for block in range(blocks):
        lead = jnp.zeros((local, lanes), jnp.float32)
        for group in range(groups):
            lead = jnp.where(group_of == group, rows_ref[block, group * local:(group + 1) * local, :], lead)
        lead_ref[block] = lead
    lead_sum_ref[...] = jnp.zeros_like(lead_sum_ref)
    row_sum_ref[...] = jnp.zeros_like(row_sum_ref)

    def scatter(image, weight, left, right):
        inner = rows_ref[right] * weight
        outer = jnp.zeros((size, lanes), jnp.float32)
        for part in range(local):
            piece = image[part * size:(part + 1) * size]
            lead_sum_ref[left, part * 8:(part + 1) * 8, :] += jnp.sum(
                (piece * inner).reshape(size // 8, 8, lanes), axis=0
            )
            outer = outer + piece * lead_ref[left, part:part + 1, :]
        row_sum_ref[right] += outer * weight

    def body(wide_acc, thin_acc):
        for queue in range(2):
            for parity in range(2):
                pltpu.matmul_pop(wide_acc[queue][parity])
                for column in range(groups):
                    pltpu.matmul_pop(thin_acc[queue][parity][column])
        arrive(0, 0)
        for slot in range(slots):
            parity = slot % 2
            raw = [index_ref[slot * 4 + axis] for axis in range(4)]
            live = jnp.where(raw[0] < blocks, 1.0, 0.0).astype(jnp.float32)
            first, second, third, fourth = [jnp.minimum(value, blocks - 1) for value in raw]
            weight = slot_weight(raw)
            inner = rows_ref[fourth] * live
            for row in range(size):
                right_ref[parity, row * size:(row + 1) * size, :] = (
                    rows_ref[third, row:row + 1, :] * inner
                ).astype(jnp.bfloat16)
            inner = rows_ref[second] * live
            packed = jnp.concatenate(
                [lead_ref[first, part:part + 1, :] * inner for part in range(local)], axis=0
            )
            left_ref[parity] = packed.T.astype(jnp.bfloat16)
            for half in range(groups // 2):
                for column in range(groups):
                    for queue in range(2):
                        line = 2 * half + queue
                        block = matrix_ref[slot, line * tile:(line + 1) * tile, column * tile:(column + 1) * tile]
                        right = right_ref[parity, column * tile:(column + 1) * tile, :]
                        right = jnp.where(group_of == line, right, jnp.zeros_like(right))
                        right = jnp.concatenate([right, jnp.zeros_like(right)], axis=1)
                        pltpu.matmul_push_rhs(right, staging_register=0, mxu_index=queue)
                        pltpu.matmul_acc_lhs(wide_acc[queue][parity], block, load_staged_rhs=0)
                        pltpu.matmul_push_rhs(block, staging_register=1, mxu_index=queue)
                        pltpu.matmul_acc_lhs(
                            thin_acc[queue][parity][column],
                            left_ref[parity, line * starts:(line + 1) * starts, :],
                            load_staged_rhs=1,
                        )
                if half + 1 < parts:
                    arrive(slot, half + 1)
                elif slot + 1 < slots:
                    arrive(slot + 1, 0)
            upper = pltpu.matmul_pop(wide_acc[0][parity])[:, :lanes] + pltpu.matmul_pop(wide_acc[1][parity])[:, :lanes]
            lower = jnp.concatenate([
                pltpu.matmul_pop(thin_acc[0][parity][column]) + pltpu.matmul_pop(thin_acc[1][parity][column])
                for column in range(groups)
            ], axis=0)
            scatter(upper, weight, first, second)
            scatter(lower.T, weight, third, fourth)

    wide = [[pltpu.ACC(queue)((tile, tile), jnp.float32) for unused in range(2)] for queue in range(2)]
    thin = [
        [[pltpu.ACC(queue)((starts, tile), jnp.float32) for unused in range(groups)] for parity in range(2)]
        for queue in range(2)
    ]
    pl.run_scoped(body, wide, thin)

    for block in range(blocks):
        lead = jnp.sum(lead_sum_ref[block].reshape(local, 8, lanes), axis=1)
        for group in range(groups):
            row_sum_ref[block, group * local:(group + 1) * local, :] += jnp.where(group_of == group, lead, 0.0)
    spread = row_sum_ref[...].reshape(order, lanes).T
    total = spread[:starts]
    for group in range(1, groups):
        total = total + spread[group * starts:(group + 1) * starts]
    y_ref[...] = total.reshape(y_ref.shape)


def apply_tensor(blocks, index, arrays, starts, order, result):
    slots, pairs = blocks.shape[:2]
    size = int(round(pairs ** 0.5))
    count = order // size
    lanes = min(pairs, 128)
    ahead = 6
    shape = jax.ShapeDtypeStruct((starts, order), jnp.float32)
    vmem = pl.BlockSpec(memory_space=pltpu.VMEM)
    groups = 128 // starts
    packed = starts % 16 == 0 and groups == 4 and pairs == 1024 and size == 32
    parts = groups // 2 if packed else 4
    settings = dict(blocks=count, size=size, parts=parts, inputs=len(arrays))
    if packed:
        kernel = functools.partial(packed_kernel, ahead=ahead, **settings)
        scratch = [
            pltpu.VMEM((count, size, lanes), jnp.float32),
            pltpu.VMEM((count, size // groups, lanes), jnp.float32),
            pltpu.VMEM((2, pairs, lanes), jnp.bfloat16),
            pltpu.VMEM((2, lanes, pairs // groups), jnp.bfloat16),
            pltpu.VMEM((count, 8 * size // groups, lanes), jnp.float32),
            pltpu.VMEM((count, size, lanes), jnp.float32),
        ]
    else:
        kernel = functools.partial(apply_kernel, **settings)
        scratch = [
            pltpu.VMEM((count, starts, pairs), jnp.float32),
            pltpu.VMEM((count, starts, lanes), jnp.float32),
            pltpu.VMEM((count, starts, pairs), jnp.float32),
            pltpu.VMEM((count, starts, lanes), jnp.float32),
        ]
    return pl.pallas_call(
        kernel,
        out_shape=(jax.ShapeDtypeStruct(result, jnp.float32), shape),
        in_specs=[pl.BlockSpec(memory_space=pltpu.SMEM), pl.BlockSpec(memory_space=pl.ANY)] + [vmem] * len(arrays),
        out_specs=(vmem, vmem),
        scratch_shapes=[pltpu.VMEM((slots, pairs, pairs), jnp.bfloat16)]
        + scratch
        + [pltpu.SemaphoreType.DMA((slots, parts))],
        compiler_params=pltpu.CompilerParams(vmem_limit_bytes=(36 if packed else 56) * 1024 * 1024),
        name="apply_tensor",
    )(index, blocks, *arrays)


def finish_kernel(offset_ref, pieces_ref, current_ref, shifts_ref, iterate_ref, estimate_ref):
    own, order = iterate_ref.shape
    image = jnp.sum(pieces_ref[...], axis=0)
    rows = pl.ds(offset_ref[0], own)
    previous = current_ref[rows, :]
    iterate_ref[...] = normalize_rows(image + shifts_ref[rows, :] * previous)
    cosine = jnp.mean(previous * image, axis=1, keepdims=True)
    estimate_ref[...] = cosine * lax.rsqrt(jnp.mean(image * image, axis=1, keepdims=True) + EPS)


def finish(offset, pieces, current, shifts, own):
    order = pieces.shape[2]
    vmem = pl.BlockSpec(memory_space=pltpu.VMEM)
    return pl.pallas_call(
        finish_kernel,
        out_shape=(
            jax.ShapeDtypeStruct((own, order), jnp.float32),
            jax.ShapeDtypeStruct((own, 1), jnp.float32),
        ),
        in_specs=[pl.BlockSpec(memory_space=pltpu.SMEM), vmem, vmem, vmem],
        out_specs=(vmem, vmem),
        compiler_params=pltpu.CompilerParams(vmem_limit_bytes=4 * 1024 * 1024),
        name="finish",
    )(offset, pieces, current, shifts)


def stage_sizes(devices):
    sizes = []
    rest = devices
    if rest % 2 == 0:
        sizes.append(2)
        rest //= 2
    while rest > 1:
        size = next(value for value in (4, 2, 3, 5, 7, rest) if rest % value == 0)
        sizes.append(size)
        rest //= size
    return sizes


def sum_terms(values, axis_name, devices):
    stride = 1
    terms = [values]
    for size in stage_sizes(devices):
        values = functools.reduce(jnp.add, terms)
        terms = [values]
        for step in reversed(range(1, size)):
            moves = []
            for device in range(devices):
                digit = device // stride % size
                target = digit ^ step if size in (2, 4) else (digit + step) % size
                moves.append((device, device + (target - digit) * stride))
            terms.append(lax.ppermute(values, axis_name, moves))
        stride *= size
    return terms


def solution(mesh):
    devices = mesh.shape["blk"]

    def body(tensor_blocks, block_index, starts, shifts):
        slots, size = tensor_blocks.shape[:2]
        own_count = starts.shape[1]
        order = starts.shape[0]
        matrices = tensor_blocks.reshape(slots, size * size, size * size)
        index = block_index.reshape(slots * 4)
        offset = lax.axis_index("blk") * own_count
        total = devices * own_count
        column = shifts[:, None]
        pieces = (devices, own_count, order)
        copies = jnp.broadcast_to(starts.T[None], pieces)
        arrays = (lax.all_to_all(copies, "blk", 0, 0, tiled=True),)
        for step in range(ITERS):
            last = step == ITERS - 1
            applied, current = apply_tensor(
                matrices, index, arrays, total, order, pieces if last else (total, order)
            )
            if not last:
                arrays = (current, column, *sum_terms(applied, "blk", devices))
        received = lax.all_to_all(applied, "blk", 0, 0, tiled=True)
        iterate, estimate = finish(offset.reshape(1), received, current, column, own_count)
        return iterate.T, estimate[:, 0]

    placed = (P("blk", None, None, None), P("blk", None), P(None, "blk"), P())
    return jax.shard_map(
        body, mesh=mesh, in_specs=placed, out_specs=(P(None, "blk"), P("blk")), check_vma=False
    )
```
